128 devices in a mesh: corpus: 16 (over y, z), neur: 8 (over x, core).
Axes of the slice: x: 4, y: 4, z: 4, core: 2. Of those that a mesh axis runs over, the one named last changes fastest.
Arguments:
- resid: bfloat16 [131072, 4096], P(('corpus', 'neur')), may hold values from -140 to 140
- norm_gain: float32 [4096], replicated, may hold values from 0.1 to 1.9
- w_gate: bfloat16 [4096, 6144], P(None, 'neur'), may hold values from -0.09375 to 0.09375
- w_up: bfloat16 [4096, 6144], P(None, 'neur'), may hold values from -0.09375 to 0.09375
- hit_neuron: int32 [8192], P(('corpus', 'neur')), may hold values from 0 to 6143, as said below
- hit_start: int32 [8192], P(('corpus', 'neur')), may hold values from 0 to 131040, as said below
- hit_mask: int32 [8192, 32], P(('corpus', 'neur')), may hold values from 0 to 1, as said below
Outputs:
- profile: float32 [8192, 32], P(('corpus', 'neur'))
- coact: float32 [8192, 768], P(('corpus', 'neur'))
The draws below stay inside these ranges and needn't reach their ends.
Inputs may be any that keep to these rules, and one draw needn't show every extreme that they name: `hit_start`: every window of 32 tokens lies inside one aligned block of 1024 corpus tokens. Among the hits of one device (blocks of 64 hits) at most 1 window lies in one such block; this bound is reached by every device in every draw. `hit_neuron`: the hits of block b of 64 hits (blocks in the order corpus+neur) name neurons of block b % 8 of 6144 // 8 neurons. `hit_mask`: the ones of each row form one run that contains positions 15 and 16.
All inputs are finite; a program needn't handle non-finite values.
Results may differ from the reference program's by a relative error of at most 0.0042.
Values may be sent and summed in bfloat16 or wider, within the bound.
A program may use at most 320 MiB of HBM per device.

```python
import math
import jax
import jax.numpy as jnp
from jax import lax

D = 4096
FF_WIN = 6144
TOK_DEV = 1024
HITS_DEV = 64
WIN = 32
CAP = 1
TOKENS = 131072
HITS = 8192
N_NEUR = 8
DEVICES = 128


def owner_table(key):
    hot_pair = jax.random.permutation(jax.random.fold_in(key, 7), DEVICES)[:2]

    def one_device(device_key):
        device_keys = jax.random.split(device_key, 3)
        hot_owner = hot_pair[jax.random.randint(device_keys[0], (), 0, 2)]
        base_ids = jnp.arange(DEVICES - 1, dtype=jnp.int32)
        other_owners = base_ids + (base_ids >= hot_owner).astype(jnp.int32)
        owner_pool = jnp.repeat(other_owners, CAP)
        chosen = owner_pool[jax.random.permutation(device_keys[1], owner_pool.shape[0])[:HITS_DEV - CAP]]
        listed = jnp.concatenate([jnp.full((CAP,), hot_owner, jnp.int32), chosen.astype(jnp.int32)])
        return listed[jax.random.permutation(device_keys[2], HITS_DEV)]
    return jax.vmap(one_device)(jax.random.split(key, DEVICES)).reshape(-1)


def draw_hit_start(key, part):
    owners = owner_table(jax.random.fold_in(key, 11))
    offsets = jax.random.randint(jax.random.fold_in(key, 12), (HITS,), 0, TOK_DEV - WIN + 1)
    return (owners * TOK_DEV + offsets).astype(jnp.int32)


def draw_hit_neuron(key, part):
    local_width = FF_WIN // N_NEUR
    block_ids = jnp.arange(HITS, dtype=jnp.int32) // HITS_DEV
    chosen = jax.random.randint(jax.random.fold_in(key, 21), (HITS,), 0, local_width)
    return (block_ids % N_NEUR * local_width + chosen).astype(jnp.int32)


def draw_hit_mask(key, part):
    first_live = jax.random.randint(jax.random.fold_in(key, 31), (HITS, 1), 0, WIN // 2)
    last_live = jax.random.randint(jax.random.fold_in(key, 32), (HITS, 1), WIN // 2, WIN)
    position = jnp.arange(WIN, dtype=jnp.int32)[None, :]
    return ((position >= first_live) & (position <= last_live)).astype(jnp.int32)


def draw_resid(key, part):
    draw_keys = jax.random.split(jax.random.fold_in(key, 41), 3)
    row_scale = jnp.exp(jax.random.uniform(draw_keys[0], (TOKENS, 1), minval=0.0, maxval=math.log(10.0)))
    column_scale = jnp.exp(jax.random.uniform(draw_keys[1], (1, D), minval=-1.0, maxval=1.0))
    values = jnp.clip(jax.random.normal(draw_keys[2], (TOKENS, D)), -5.0, 5.0)
    return (values * row_scale * column_scale).astype(jnp.bfloat16)


def block_levels(own_key, shape, cuts, least, top_value):
    def one(dim, shards_of):
        steps = jax.random.uniform(jax.random.fold_in(jax.random.fold_in(own_key, 6), dim), (shards_of,), jnp.float32, least / len(cuts), top_value / len(cuts))
        return jnp.repeat(jnp.exp(steps), shape[dim] // shards_of).reshape((-1,) + (1,) * (len(shape) - dim - 1))

    level = one(*cuts[0])
    for cut in cuts[1:]:
        level = level * one(*cut)
    return level


def normal_values(key, dims, width, most, shards=(), kind=jnp.bfloat16):
    result = width * jax.random.normal(key, dims, jnp.float32)
    if shards:
        result = result * block_levels(key, dims, shards, -0.22, 0.18)
    return jnp.clip(result, -most, most).astype(kind)


def setup_inputs(seed: int = 0) -> dict:
    arg_keys = jax.random.split(jax.random.key(seed), 8)
    return {
        "resid": draw_resid(jax.random.fold_in(arg_keys[7], 71), 0),
        "norm_gain": jnp.clip(1.0 + 0.18 * jax.random.normal(arg_keys[1], (D,), jnp.float32), 0.1, 1.9),
        "w_gate": normal_values(arg_keys[2], (D, FF_WIN), D ** -0.5, 0.09375, ((1, 8),)),
        "w_up": normal_values(arg_keys[3], (D, FF_WIN), D ** -0.5, 0.09375, ((1, 8),)),
        "hit_neuron": draw_hit_neuron(jax.random.fold_in(arg_keys[7], 71), 0),
        "hit_start": draw_hit_start(jax.random.fold_in(arg_keys[7], 71), 0),
        "hit_mask": draw_hit_mask(jax.random.fold_in(arg_keys[7], 71), 0),
    }


EPS = 1e-05

def activations(rows, norm_gain, w_gate, w_up):
    values = rows.astype(jnp.float32)
    power = lax.optimization_barrier(jnp.mean(values * values, axis=-1, keepdims=True))
    normed = (values * lax.rsqrt(power + EPS) * norm_gain).astype(jnp.bfloat16)
    gate = jnp.dot(normed, w_gate, preferred_element_type=jnp.float32)
    upward = jnp.dot(normed, w_up, preferred_element_type=jnp.float32)
    return jax.nn.silu(gate) * upward

def reference(resid, norm_gain, w_gate, w_up, hit_neuron, hit_start, hit_mask):
    local_width = FF_WIN // N_NEUR

    def take_window(begin):
        return lax.dynamic_slice_in_dim(resid, begin, WIN, 0)

    def one_group(inputs):
        index, starts, masks, neurons = inputs
        block = (index % N_NEUR).astype(jnp.int32)
        first = (block * local_width).astype(jnp.int32)
        gate_cols = lax.dynamic_slice_in_dim(w_gate, first, local_width, 1)
        up_cols = lax.dynamic_slice_in_dim(w_up, first, local_width, 1)
        windows = jax.vmap(take_window)(starts)
        acts = activations(windows.reshape(HITS_DEV * WIN, D), norm_gain, gate_cols, up_cols).reshape(HITS_DEV, WIN, local_width)
        live = masks > 0
        coact = lax.optimization_barrier(jnp.max(jnp.where(live[:, :, None], acts, -jnp.inf), axis=1))
        local = (neurons - first).astype(jnp.int32)
        picked = jnp.take_along_axis(acts, local[:, None, None], axis=2)[:, :, 0]
        return (picked * masks.astype(jnp.float32), coact)
    groups = HITS // HITS_DEV
    profile, coact = lax.map(one_group, (jnp.arange(groups, dtype=jnp.int32), hit_start.reshape(groups, HITS_DEV), hit_mask.reshape(groups, HITS_DEV, WIN), hit_neuron.reshape(groups, HITS_DEV)))
    return (profile.reshape(HITS, WIN), coact.reshape(HITS, local_width))
```

```python
import functools

import jax
import jax.numpy as jnp
from jax import lax
from jax.experimental import pallas as pl
from jax.experimental.pallas import tpu as pltpu
from jax.sharding import PartitionSpec as P

EPS = 1e-05
MESH = pl.DeviceIdType.MESH
ANY = pl.BlockSpec(memory_space=pl.ANY)
TILE = 8
GROUP = 8
SPAN = 5
CHUNK_TILES = (56, 56, 16)


def norm_body(bounds, x_ref, g_ref, *outs):
    i = pl.program_id(0)
    v = x_ref[...].astype(jnp.float32)
    power = jnp.mean(v * v, axis=-1, keepdims=True)
    r = (v * lax.rsqrt(power + EPS) * g_ref[...]).astype(jnp.bfloat16)
    r = r.reshape(outs[0].shape)
    for q, out in enumerate(outs):

        @pl.when((i >= bounds[q]) & (i < bounds[q + 1]))
        def _(out=out):
            out[...] = r


def normalise(resid, gain):
    rows, width = resid.shape
    step = 8
    bounds = [0]
    for t in CHUNK_TILES:
        bounds.append(bounds[-1] + t // step)

    def out_map(q):
        lo, hi = bounds[q], bounds[q + 1]
        return lambda i: (jnp.clip(i - lo, 0, hi - lo - 1), 0, 0)

    return pl.pallas_call(
        functools.partial(norm_body, bounds),
        grid=(bounds[-1],),
        in_specs=[
            pl.BlockSpec((step * TILE, width), lambda i: (i, 0)),
            pl.BlockSpec((1, width), lambda i: (0, 0)),
        ],
        out_specs=[
            pl.BlockSpec((step, TILE, width), out_map(q))
            for q in range(len(CHUNK_TILES))
        ],
        out_shape=[
            jax.ShapeDtypeStruct((t, TILE, width), jnp.bfloat16) for t in CHUNK_TILES
        ],
        cost_estimate=pl.CostEstimate(
            flops=8 * rows * width, bytes_accessed=4 * rows * width, transcendentals=0
        ),
        name="normalise",
    )(resid, gain.reshape(1, width))


def stage_body(cfg, *refs):
    chunks, owners, last_part, width, cols = cfg
    n_src = len(owners) * len(chunks)
    tbl = refs[0]
    srcs = refs[1 : 1 + n_src]
    wg, wu = refs[1 + n_src : 3 + n_src]
    n_in = 3 + n_src
    co_ref, pr_ref = refs[n_in : n_in + 2]
    lhs, wbuf, act, picked, wsem, lsem = refs[n_in + 2 :]
    n_own = len(owners)
    slots = 16 * n_own

    wcopies = [
        pltpu.make_async_copy(wg, wbuf.at[:, pl.ds(0, cols)], wsem.at[0]),
        pltpu.make_async_copy(wu, wbuf.at[:, pl.ds(cols, cols)], wsem.at[1]),
    ]
    for c in wcopies:
        c.start()

    edge = sum(CHUNK_TILES[:-1])

    def scan(s, n):
        start = tbl[4 * s]
        ok = start >= 0
        if last_part == 0:
            ok = ok & (lax.div(start, TILE) + SPAN <= edge)
        elif last_part == 1:
            ok = ok & (lax.div(start, TILE) + SPAN > edge)

        @pl.when(ok)
        def _():
            picked[n] = s

        return n + ok.astype(jnp.int32)

    count = lax.fori_loop(0, slots, scan, jnp.int32(0))
    batches = lax.div(count + GROUP - 1, GROUP)

    def slot_of(batch, w):
        return picked[jnp.minimum(batch * GROUP + w, count - 1)]

    starts = [0]
    for t in CHUNK_TILES:
        starts.append(starts[-1] + t)

    def fetch(batch):
        buf = lax.rem(batch, 2)

        def window(w, carry):
            s = slot_of(batch, w)
            u = lax.rem(s, n_own)
            tile0 = jnp.minimum(lax.div(tbl[4 * s], TILE), starts[-1] - SPAN)

            def one(k, carry):
                t = tile0 + k
                for a in range(n_own):
                    for b, q in enumerate(chunks):
                        cond = (t >= starts[q]) & (t < starts[q + 1])
                        if n_own > 1:
                            cond = cond & (u == a)

                        @pl.when(cond)
                        def _(a=a, b=b, q=q):
                            pltpu.make_async_copy(
                                srcs[a * len(chunks) + b].at[t - starts[q]],
                                lhs.at[buf, w * SPAN + k],
                                lsem.at[buf],
                            ).start()

                return carry

            return lax.fori_loop(0, SPAN, one, carry)

        lax.fori_loop(0, GROUP, window, 0)

    @pl.when(count > 0)
    def _():
        fetch(jnp.int32(0))

    for c in wcopies:
        c.wait()
    pr_ref[...] = jnp.zeros_like(pr_ref)

    rows = GROUP * SPAN * TILE
    nt = 256
    row_ids = lax.broadcasted_iota(jnp.int32, (SPAN * TILE, 1), 0)
    lane_ids = lax.broadcasted_iota(jnp.int32, (SPAN * TILE, nt), 1)
    slot_lane = lax.broadcasted_iota(jnp.int32, pr_ref.shape, 1)

    def run(batch, carry):
        @pl.when(batch + 1 < batches)
        def _():
            fetch(batch + 1)

        buf = lax.rem(batch, 2)
        pltpu.make_async_copy(
            srcs[0].at[pl.ds(0, GROUP * SPAN)], lhs.at[buf], lsem.at[buf]
        ).wait()
        x = lhs.at[buf]

        def cols_step(j, carry):
            lo = pl.multiple_of(j * nt, nt)
            left = x[...].reshape(rows, width)
            gate = jnp.dot(
                left, wbuf[:, pl.ds(lo, nt)], preferred_element_type=jnp.float32
            )
            up = jnp.dot(
                left,
                wbuf[:, pl.ds(pl.multiple_of(lo + cols, nt), nt)],
                preferred_element_type=jnp.float32,
            )
            act[...] = gate / (1.0 + jnp.exp(-gate)) * up

            def window(w, carry):
                s = slot_of(batch, w)
                start = tbl[4 * s]
                neuron = tbl[4 * s + 1]
                first = tbl[4 * s + 2]
                last = tbl[4 * s + 3]
                tile0 = jnp.minimum(lax.div(start, TILE), starts[-1] - SPAN)
                shift = start - tile0 * TILE
                a = act[pl.ds(pl.multiple_of(w * SPAN * TILE, TILE), SPAN * TILE), :]
                live = (row_ids >= shift + first) & (row_ids <= shift + last)
                top = jnp.max(jnp.where(live, a, -jnp.inf), axis=0, keepdims=True)
                co_ref[pl.ds(s, 1), pl.ds(lo, nt)] = top
                col = jnp.sum(
                    jnp.where(lane_ids == neuron - lo, a, 0.0), axis=1, keepdims=True
                )
                mine = (neuron >= lo) & (neuron < lo + nt)
                pr_ref[...] = jnp.where((slot_lane == s) & mine, col, pr_ref[...])
                return carry

            lax.fori_loop(0, GROUP, window, 0)
            return carry

        lax.fori_loop(0, cols // nt, cols_step, 0)
        return carry

    lax.fori_loop(0, batches, run, 0)


def stage(tbl, sources, chunks, last_part, wg, wu, share, name):
    width, cols = wg.shape
    n_own = len(sources)
    slots = 16 * n_own
    flat = [sources[a][q] for a in range(n_own) for q in chunks]
    cfg = (tuple(chunks), tuple(range(n_own)), last_part, width, cols)
    rows = GROUP * SPAN * TILE
    flops = int(share * 2048 * 1.25 * 4 * width * cols)
    return pl.pallas_call(
        functools.partial(stage_body, cfg),
        in_specs=[pl.BlockSpec(memory_space=pltpu.SMEM)] + [ANY] * (len(flat) + 2),
        out_specs=[pl.BlockSpec(memory_space=pltpu.VMEM)] * 2,
        out_shape=[
            jax.ShapeDtypeStruct((slots, cols), jnp.float32),
            jax.ShapeDtypeStruct((SPAN * TILE, 128), jnp.float32),
        ],
        scratch_shapes=[
            pltpu.VMEM((2, GROUP * SPAN, TILE, width), jnp.bfloat16),
            pltpu.VMEM((width, 2 * cols), jnp.bfloat16),
            pltpu.VMEM((rows, 256), jnp.float32),
            pltpu.SMEM((slots,), jnp.int32),
            pltpu.SemaphoreType.DMA((2,)),
            pltpu.SemaphoreType.DMA((2,)),
        ],
        compiler_params=pltpu.CompilerParams(vmem_limit_bytes=40 * 1024 * 1024),
        cost_estimate=pl.CostEstimate(
            flops=flops, bytes_accessed=4 * width * cols, transcendentals=0
        ),
        name=name,
    )(tbl, *flat, wg, wu)


def exchange_body(pay_ref, got_ref, send_sems, recv_sems):
    c = lax.axis_index("corpus")
    n = lax.axis_index("neur")
    groups = pay_ref.shape[0] // 2

    barrier = pltpu.get_barrier_semaphore()

    def peer(k):
        b = k // groups
        return {
            "corpus": lax.rem(c + k % groups, groups),
            "neur": lax.rem(n + 4 * b, 8),
        }, b

    for k in range(1, 2 * groups):
        dev, _ = peer(k)
        pl.semaphore_signal(barrier, inc=1, device_id=dev, device_id_type=MESH)
    pl.semaphore_wait(barrier, 2 * groups - 1)

    copies = []
    for k in range(1, 2 * groups):
        dev, b = peer(k)
        copies.append(
            pltpu.make_async_remote_copy(
                src_ref=pay_ref.at[b * groups + dev["corpus"]],
                dst_ref=got_ref.at[b * groups + c],
                send_sem=send_sems.at[k],
                recv_sem=recv_sems.at[k],
                device_id=dev,
                device_id_type=MESH,
            )
        )
        copies[-1].start()
    got_ref[pl.ds(c, 1)] = pay_ref[pl.ds(c, 1)]
    for copy in copies:
        copy.wait()


def exchange(pay):
    peers = pay.shape[0]
    return pl.pallas_call(
        exchange_body,
        in_specs=[pl.BlockSpec(memory_space=pltpu.VMEM)],
        out_specs=pl.BlockSpec(memory_space=pltpu.VMEM),
        out_shape=jax.ShapeDtypeStruct(pay.shape, pay.dtype),
        scratch_shapes=[
            pltpu.SemaphoreType.DMA((peers,)),
            pltpu.SemaphoreType.DMA((peers,)),
        ],
        compiler_params=pltpu.CompilerParams(collective_id=0, has_side_effects=True),
        name="results",
    )(pay)


def per_device(resid, norm_gain, w_gate, w_up, hit_neuron, hit_start, hit_mask):
    block_rows = resid.shape[0]
    width, cols = w_gate.shape
    own_hits, win = hit_mask.shape
    c = lax.axis_index("corpus")
    n = lax.axis_index("neur")
    x, core = n // 2, n % 2

    def along_x(hops):
        return [
            (m, ((m // 2 + (hops if m % 2 == 0 else 4 - hops)) % 4) * 2 + m % 2)
            for m in range(8)
        ]

    hop, swap = along_x(1), [(m, m ^ 1) for m in range(8)]

    depth = width // 16
    parts = [lax.dynamic_slice_in_dim(w, c * depth, depth, 0) for w in (w_gate, w_up)]
    once = [lax.ppermute(p, "neur", hop) for p in parts]
    twice = [lax.ppermute(p, "neur", hop) for p in once]
    other = [lax.all_gather(p, "corpus", axis=0, tiled=True) for p in twice]

    half = win // 2
    first = half - jnp.sum(hit_mask[:, :half], axis=1)
    last = half - 1 + jnp.sum(hit_mask[:, half:], axis=1)
    info = jnp.stack([hit_start, hit_neuron - n * cols, first, last])
    info = lax.all_gather(info, ("corpus", "neur"), axis=0, tiled=False)
    info = info.reshape(16, 8, 4, own_hits)
    mine = jnp.stack(
        [
            lax.dynamic_index_in_dim(info, n, 1, keepdims=False),
            lax.dynamic_index_in_dim(info, (n + 4) % 8, 1, keepdims=False),
        ]
    )
    ahead, behind = (x + 1) % 4, (x + 3) % 4
    from_c0, from_c1 = behind * 2, ahead * 2 + 1
    owners = jnp.stack(
        [
            n,
            n ^ 1,
            jnp.where(core == 0, from_c0, from_c1),
            jnp.where(core == 0, from_c1, from_c0),
        ]
    )
    owners = (c * 8 + owners) * block_rows
    local = mine[:, :, 0][:, :, None, :] - owners[None, None, :, None]
    match = (local >= 0) & (local < block_rows)

    def pick(field):
        return jnp.sum(jnp.where(match, field, 0), axis=-1)

    found = jnp.any(match, axis=-1)
    tbl = jnp.stack(
        [jnp.where(found, pick(local), -1)]
        + [pick(mine[:, :, f][:, :, None, :]) for f in (1, 2, 3)],
        axis=-1,
    )

    def table(b, u):
        return tbl[b, :, 2 * u : 2 * u + 2].reshape(-1)

    rows = normalise(resid, norm_gain)
    rows, _ = lax.optimization_barrier((rows, once))
    near = [rows, [lax.ppermute(r, "neur", swap) for r in rows]]
    got = [lax.ppermute(r, "neur", hop) for r in rows]
    far = [got, [lax.ppermute(r, "neur", swap) for r in got]]

    every, early = (0, 1, 2), (0, 1)
    own_a = stage(table(0, 0), near, every, None, w_gate, w_up, 0.25, "own_a")
    far_a = stage(table(0, 1), far, early, 0, w_gate, w_up, 0.21, "far_a")
    own_b = stage(table(1, 0), near, every, None, *other, 0.25, "own_b")
    far_b = stage(table(1, 1), far, early, 0, *other, 0.21, "far_b")
    end_a = stage(table(0, 1), far, (1, 2), 1, w_gate, w_up, 0.04, "end_a")
    end_b = stage(table(1, 1), far, (1, 2), 1, *other, 0.04, "end_b")

    edge = sum(CHUNK_TILES[:-1])

    def merged(b, early_part, late_part):
        late = (tbl[b, :, 2:, 0] // TILE + SPAN > edge).reshape(-1)
        top = jnp.where(late[:, None], late_part[0], early_part[0])
        prof = jnp.where(late[None, :], late_part[1][:, :32], early_part[1][:, :32])
        return top, prof

    tops, profs = [], []
    for b, own, early_part, late_part in ((0, own_a, far_a, end_a), (1, own_b, far_b, end_b)):
        far_top, far_prof = merged(b, early_part, late_part)
        tops.append(
            jnp.concatenate(
                [own[0].reshape(16, 2, cols), far_top.reshape(16, 2, cols)], axis=1
            )
        )
        prof = jnp.concatenate(
            [
                own[1][:, :32].T.reshape(16, 2, SPAN * TILE),
                far_prof.T.reshape(16, 2, SPAN * TILE),
            ],
            axis=1,
        )
        profs.append(jnp.pad(prof, ((0, 0), (0, 0), (0, 128 - SPAN * TILE))))
    pay = jnp.concatenate([jnp.stack(tops), jnp.stack(profs)], axis=-1)
    pay = pay.reshape(32, 4, cols + 128)
    back = exchange(pay).reshape(128, cols + 128)

    owner = hit_start // block_rows
    at_c, at_n = owner // 8, owner % 8
    at_x, at_core = at_n // 2, at_n % 2
    same = (at_x % 2) == (x % 2)
    comp_x = jnp.where(same, at_x, (at_x + jnp.where(at_core == 0, 1, 3)) % 4)
    far_block = (comp_x != x).astype(jnp.int32)
    role = jnp.where(same, 0, 2) + (at_core != core).astype(jnp.int32)
    place = (far_block * 16 + at_c) * 4 + role
    mine_back = jnp.take(back, place, axis=0, mode="clip")
    coact = mine_back[:, :cols]
    wide = mine_back[:, cols : cols + SPAN * TILE]
    within = hit_start % block_rows
    shift = within - jnp.minimum(within // TILE, block_rows // TILE - SPAN) * TILE
    profile = jnp.zeros((own_hits, win), jnp.float32)
    for s in range(TILE + 1):
        profile = jnp.where((shift == s)[:, None], wide[:, s : s + win], profile)
    live = hit_mask.astype(jnp.float32)
    return (jnp.where(hit_mask > 0, profile * live, 0.0), coact)


def solution(mesh):
    placed = (
        P(("corpus", "neur"), None),
        P(),
        P(None, "neur"),
        P(None, "neur"),
        P(("corpus", "neur")),
        P(("corpus", "neur")),
        P(("corpus", "neur"), None),
    )
    return jax.shard_map(
        per_device,
        mesh=mesh,
        in_specs=placed,
        out_specs=(P(("corpus", "neur"), None), P(("corpus", "neur"), None)),
        check_vma=False,
    )
```
